64 devices in a mesh: rep: 4 (over x, y), grp: 16 (over z, core).
Axes of the slice: x: 2, y: 2, z: 8, core: 2. Of those that a mesh axis runs over, the one named last changes fastest.
The devices are a block of a 4x4x8 slice.
Arguments:
- x_in: bfloat16 [2048, 4096], P(('rep', 'grp')), parts along dimension 0
- seq_len: int32 [2048], P(('rep', 'grp')), parts along dimension 0
- k_cache: bfloat16 [2048, 256, 2, 128], P(('rep', 'grp')), parts along dimension 0
- v_cache: bfloat16 [2048, 256, 2, 128], P(('rep', 'grp')), parts along dimension 0
- gamma_attn: bfloat16 [4096], replicated
- w_qkv: bfloat16 [4096, 4608], replicated
- b_qkv: bfloat16 [4608], replicated
- w_proj: bfloat16 [4096, 4096], replicated
- gamma_mlp: bfloat16 [4096], replicated
- w_in: bfloat16 [2, 13696, 4096], P(None, 'grp')
- w_out: bfloat16 [13696, 4096], P('grp')
Outputs:
- output 1: bfloat16 [2048, 4096], P(('rep', 'grp')), parts along dimension 0
- output 2: bfloat16 [2048, 256, 2, 128], P(('rep', 'grp')), parts along dimension 0
- output 3: bfloat16 [2048, 256, 2, 128], P(('rep', 'grp')), parts along dimension 0
There are 4 independent parts. The reference program is written for one: setup_inputs(seed, part) draws one part's arguments, and reference() takes and returns one part's arrays. A program takes and returns all parts, laid end to end along the dimension named above; an argument that names none is the same for every part.
All inputs are finite; a program needn't handle non-finite values.
Results may differ from the reference program's by a relative error of at most 0.0102376.
Values are sent between devices in bfloat16 or wider.
A program may use at most 768 MiB of HBM per device.

```python
import jax
import jax.numpy as jnp
from jax import lax

HIDDEN = 4096
HEADS = 32
KV_HEADS = 2
HEAD = 128
FFN = 13696
LMAX = 256
BATCH = 512
ROPE_BASE = 10000
QKV_WIDTH = (HEADS + 2 * KV_HEADS) * HEAD
ROT_DIM = HEAD // 2
EPS = 1e-5


def setup_inputs(seed: int = 0, part: int = 0) -> dict:
    keys = jax.random.split(jax.random.key(seed), 10)
    gamma_attn = (1.0 + 0.3 * jax.random.normal(keys[0], (HIDDEN,), jnp.float32)).astype(jnp.bfloat16)
    w_qkv = (jax.random.normal(keys[1], (HIDDEN, QKV_WIDTH), jnp.float32) * HIDDEN ** -0.5).astype(jnp.bfloat16)
    b_qkv = (0.5 * jax.random.normal(keys[2], (QKV_WIDTH,), jnp.float32)).astype(jnp.bfloat16)
    w_proj = (jax.random.normal(keys[3], (HEADS * HEAD, HIDDEN), jnp.float32) * (HEADS * HEAD) ** -0.5).astype(jnp.bfloat16)
    gamma_mlp = (1.0 + 0.3 * jax.random.normal(keys[4], (HIDDEN,), jnp.float32)).astype(jnp.bfloat16)
    w_in = (jax.random.normal(keys[5], (2, FFN, HIDDEN), jnp.float32) * HIDDEN ** -0.5).astype(jnp.bfloat16)
    w_out = (jax.random.normal(keys[6], (FFN, HIDDEN), jnp.float32) * FFN ** -0.5).astype(jnp.bfloat16)
    x_in = jax.random.normal(jax.random.fold_in(keys[7], part), (BATCH, HIDDEN), jnp.float32).astype(jnp.bfloat16)
    seq_len = jax.random.randint(jax.random.fold_in(keys[8], part), (BATCH,), 1, LMAX, dtype=jnp.int32)
    seq_len = seq_len.at[0].set(LMAX - 1).at[BATCH - 1].set(1)
    cache_keys = jax.random.split(jax.random.fold_in(keys[9], part), 3)
    cache_shape = (BATCH, LMAX, KV_HEADS, HEAD)
    k_cache = (2.0 * jax.random.normal(cache_keys[0], cache_shape, jnp.float32)).astype(jnp.bfloat16)
    drift = jnp.cumsum(jax.random.normal(cache_keys[1], cache_shape, jnp.float32), axis=1) * LMAX ** -0.5
    v_cache = (drift + jax.random.normal(cache_keys[2], cache_shape, jnp.float32)).astype(jnp.bfloat16)
    return {'x_in': x_in, 'seq_len': seq_len, 'k_cache': k_cache, 'v_cache': v_cache,
            'gamma_attn': gamma_attn, 'w_qkv': w_qkv, 'b_qkv': b_qkv, 'w_proj': w_proj,
            'gamma_mlp': gamma_mlp, 'w_in': w_in, 'w_out': w_out}


def rms_norm(vals, gain):
    mean_sq = jnp.mean(vals * vals, axis=-1, keepdims=True)
    return (vals * lax.rsqrt(mean_sq + EPS) * gain.astype(jnp.float32)).astype(jnp.bfloat16)


def rotary(vals, positions):
    inv_freq = ROPE_BASE ** (-jnp.arange(0, ROT_DIM, 2, dtype=jnp.float32) / ROT_DIM)
    angles = positions.astype(jnp.float32)[:, None] * inv_freq[None, :]
    cosine = jnp.cos(angles)[:, None, :]
    sine = jnp.sin(angles)[:, None, :]
    pairs = vals[..., :ROT_DIM].reshape(vals.shape[:-1] + (ROT_DIM // 2, 2))
    even_part = pairs[..., 0]
    odd_part = pairs[..., 1]
    rotated = jnp.stack([even_part * cosine - odd_part * sine, odd_part * cosine + even_part * sine], axis=-1)
    return jnp.concatenate([rotated.reshape(vals.shape[:-1] + (ROT_DIM,)), vals[..., ROT_DIM:]], axis=-1)


def reference(x_in, seq_len, k_cache, v_cache, gamma_attn, w_qkv, b_qkv, w_proj, gamma_mlp, w_in, w_out):
    x_f32 = x_in.astype(jnp.float32)
    normed = rms_norm(x_f32, gamma_attn)
    qkv_proj = jnp.dot(normed, w_qkv, preferred_element_type=jnp.float32) + b_qkv.astype(jnp.float32)
    q_width = HEADS * HEAD
    kv_width = KV_HEADS * HEAD
    query_rot = rotary(qkv_proj[:, :q_width].reshape(BATCH, HEADS, HEAD), seq_len).astype(jnp.bfloat16)
    key_new = rotary(qkv_proj[:, q_width:q_width + kv_width].reshape(BATCH, KV_HEADS, HEAD), seq_len).astype(jnp.bfloat16)
    value_new = qkv_proj[:, q_width + kv_width:].reshape(BATCH, KV_HEADS, HEAD).astype(jnp.bfloat16)
    positions = jnp.arange(LMAX, dtype=jnp.int32)
    at_len = (positions[None, :] == seq_len[:, None])[:, :, None, None]
    k_out = jnp.where(at_len, key_new[:, None], k_cache)
    v_out = jnp.where(at_len, value_new[:, None], v_cache)

    def one_seq(seq_args):
        q_row, k_row, v_row, length = seq_args
        q_grouped = q_row.reshape(KV_HEADS, HEADS // KV_HEADS, HEAD).astype(jnp.float32)
        attn_scores = jnp.einsum('gqd,lgd->gql', q_grouped, k_row.astype(jnp.float32)) * HEAD ** -0.5
        attn_scores = jnp.where((positions <= length)[None, None, :], attn_scores, -jnp.inf)
        attn_probs = jax.nn.softmax(attn_scores, axis=-1).astype(jnp.bfloat16)
        context = jnp.einsum('gql,lgd->gqd', attn_probs.astype(jnp.float32), v_row.astype(jnp.float32))
        return context.reshape(HEADS * HEAD).astype(jnp.bfloat16)

    context = lax.map(one_seq, (query_rot, k_out, v_out, seq_len))
    hidden = x_f32 + jnp.dot(context, w_proj, preferred_element_type=jnp.float32)
    mlp_in = rms_norm(hidden, gamma_mlp)
    gate_up = jnp.dot(mlp_in, w_in.reshape(2 * FFN, HIDDEN).T, preferred_element_type=jnp.float32)
    swiglu = (jax.nn.silu(gate_up[:, :FFN]) * gate_up[:, FFN:]).astype(jnp.bfloat16)
    mlp_out = jnp.dot(swiglu, w_out, preferred_element_type=jnp.float32)
    layer_out = (hidden + mlp_out).astype(jnp.bfloat16)
    return (layer_out, k_out, v_out)
```

```python
import functools

import jax
import jax.numpy as jnp
from jax import lax
from jax.experimental import pallas as pl
from jax.experimental.pallas import tpu as pltpu
from jax.sharding import PartitionSpec as P

HEAD_DIM = 128
ROPE_BASE = 10000.0
EPS = 1e-5
MESH = pl.DeviceIdType.MESH
LANES = 128


def rms_norm(vals, gain):
    mean_sq = jnp.mean(vals * vals, axis=-1, keepdims=True)
    return (vals * lax.rsqrt(mean_sq + EPS) * gain.astype(jnp.float32)).astype(jnp.bfloat16)


def rotary(vals, positions):
    rot_dim = HEAD_DIM // 2
    inv_freq = ROPE_BASE ** (-jnp.arange(0, rot_dim, 2, dtype=jnp.float32) / rot_dim)
    angles = positions.astype(jnp.float32)[:, None] * inv_freq[None, :]
    cosine = jnp.cos(angles)[:, None, :]
    sine = jnp.sin(angles)[:, None, :]
    pairs = vals[..., :rot_dim].reshape(vals.shape[:-1] + (rot_dim // 2, 2))
    even_part = pairs[..., 0]
    odd_part = pairs[..., 1]
    rotated = jnp.stack([even_part * cosine - odd_part * sine, odd_part * cosine + even_part * sine], axis=-1)
    return jnp.concatenate([rotated.reshape(vals.shape[:-1] + (rot_dim,)), vals[..., rot_dim:]], axis=-1)


def attention_block(x_in, seq_len, k_cache, v_cache, gamma_attn, w_qkv, b_qkv, w_proj):
    batch_rows, cache_len, kv_heads = k_cache.shape[0], k_cache.shape[1], k_cache.shape[2]
    num_heads = w_proj.shape[0] // HEAD_DIM
    q_width = num_heads * HEAD_DIM
    kv_width = kv_heads * HEAD_DIM
    x_f32 = x_in.astype(jnp.float32)
    normed = rms_norm(x_f32, gamma_attn)
    qkv_proj = jnp.dot(normed, w_qkv, preferred_element_type=jnp.float32) + b_qkv.astype(jnp.float32)
    query_rot = rotary(qkv_proj[:, :q_width].reshape(batch_rows, num_heads, HEAD_DIM), seq_len).astype(jnp.bfloat16)
    key_new = rotary(qkv_proj[:, q_width:q_width + kv_width].reshape(batch_rows, kv_heads, HEAD_DIM), seq_len).astype(jnp.bfloat16)
    value_new = qkv_proj[:, q_width + kv_width:].reshape(batch_rows, kv_heads, HEAD_DIM).astype(jnp.bfloat16)
    positions = jnp.arange(cache_len, dtype=jnp.int32)
    at_len = (positions[None, :] == seq_len[:, None])[:, :, None, None]
    k_out = jnp.where(at_len, key_new[:, None], k_cache)
    v_out = jnp.where(at_len, value_new[:, None], v_cache)
    q_grouped = query_rot.reshape(batch_rows, kv_heads, num_heads // kv_heads, HEAD_DIM)
    attn_scores = jnp.einsum('bgqd,blgd->bgql', q_grouped, k_out, preferred_element_type=jnp.float32) * HEAD_DIM ** -0.5
    visible = (positions[None, :] <= seq_len[:, None])[:, None, None, :]
    attn_probs = jax.nn.softmax(jnp.where(visible, attn_scores, -jnp.inf), axis=-1).astype(jnp.bfloat16)
    context = jnp.einsum('bgql,blgd->bgqd', attn_probs, v_out, preferred_element_type=jnp.float32)
    context = context.astype(jnp.bfloat16).reshape(batch_rows, q_width)
    hidden = x_f32 + jnp.dot(context, w_proj, preferred_element_type=jnp.float32)
    return hidden, k_out, v_out


def mlp_kernel(chips, m_ref, h_ref, w_in_ref, w_out_ref, o_ref, m_all, w1, w2, act, part, pair_rx, rs_rx, rs_tx,
               w1_sem, w2_sem, ag_send, ag_recv, pt_send, pt_recv, px_send, px_recv, rs_send, rs_recv):
    f32, bf16 = jnp.float32, jnp.bfloat16
    width = m_ref.shape[1]
    half = width // 2
    rb = m_ref.shape[0] // 2
    ffn = w_out_ref.shape[0]
    fblocks = w2.shape[0] // LANES
    far = chips // 2
    ncol = 512

    me = lax.axis_index('grp')
    z, core = me // 2, me % 2
    other = 1 - core
    right = lax.rem(z + 1, chips) * 2 + core
    left = lax.rem(z + chips - 1, chips) * 2 + core
    partner = z * 2 + other
    nbr = (right, left)

    def chip_at(direction, k):
        return lax.rem(z + (chips - k if direction == 0 else k), chips)

    def rows(c, chip):
        return pl.ds(pl.multiple_of((c * chips + chip) * rb, rb), rb)

    def rcopy(src, dst, ssem, rsem, dev):
        return pltpu.make_async_remote_copy(src_ref=src, dst_ref=dst, send_sem=ssem, recv_sem=rsem,
                                            device_id={'grp': dev}, device_id_type=MESH)

    w_copies = []
    for j in range(fblocks):
        n = min(LANES, ffn - j * LANES)
        for c in range(2):
            w_copies.append(pltpu.make_async_copy(w_in_ref.at[c, pl.ds(j * LANES, n), :],
                                                  w1.at[pl.ds((2 * j + c) * LANES, n), :], w1_sem.at[2 * j + c]))
    w_copies.append(pltpu.make_async_copy(w_out_ref, w2.at[pl.ds(0, ffn), :], w2_sem))

    barrier = pltpu.get_barrier_semaphore()
    for dev in (right, left, partner):
        pl.semaphore_signal(barrier, inc=1, device_id={'grp': dev}, device_id_type=MESH)
    pl.semaphore_wait(barrier, 3)

    def ag_cols(direction, k):
        return pl.ds(direction * half, half) if k == far else pl.ds(0, width)

    def ag(b, direction, k):
        cols = ag_cols(direction, k)
        if k == 1:
            src = m_ref.at[pl.ds(b * rb, rb), :]
            sent = z
        else:
            sent = chip_at(direction, k - 1)
            src = m_all.at[b, rows(core, sent), cols]
        return rcopy(src, m_all.at[b, rows(core, sent), cols], ag_send.at[b, direction, k - 1],
                     ag_recv.at[b, direction, k - 1], nbr[direction])

    def ag_wait(b, direction, k):
        got = m_all.at[b, rows(core, chip_at(direction, k)), ag_cols(direction, k)]
        rcopy(got, got, ag_send.at[b, direction, k - 1], ag_recv.at[b, direction, k - 1], nbr[direction]).wait_recv()

    def pt(b, direction, k):
        if k == 0:
            blk = m_all.at[b, rows(core, z), :]
            return rcopy(m_ref.at[pl.ds(b * rb, rb), :], blk, pt_send.at[b, 0], pt_recv.at[b, 0], partner)
        slot = 1 + direction * far + k - 1
        blk = m_all.at[b, rows(core, chip_at(direction, k)), ag_cols(direction, k)]
        return rcopy(blk, blk, pt_send.at[b, slot], pt_recv.at[b, slot], partner)

    def pt_wait(b, direction, k):
        if k == 0:
            blk = m_all.at[b, rows(other, z), :]
            return rcopy(blk, blk, pt_send.at[b, 0], pt_recv.at[b, 0], partner).wait_recv()
        slot = 1 + direction * far + k - 1
        blk = m_all.at[b, rows(other, chip_at(direction, k)), ag_cols(direction, k)]
        return rcopy(blk, blk, pt_send.at[b, slot], pt_recv.at[b, slot], partner).wait_recv()

    started = []

    def start(copy):
        copy.start()
        started.append(copy)

    for b in range(2):
        for d in range(2):
            start(ag(b, d, 1))
    for b in range(2):
        start(pt(b, 0, 0))
    for copy in w_copies:
        copy.start()
    for b in range(2):
        m_all[b, rows(core, z), :] = m_ref[pl.ds(b * rb, rb), :]
    for k in range(1, far + 1):
        for b in range(2):
            for d in range(2):
                ag_wait(b, d, k)
                if k < far:
                    start(ag(b, d, k + 1))
                start(pt(b, d, k))
    for copy in w_copies:
        copy.wait()
    edge = ffn // 16 * 16
    if edge < w2.shape[0]:
        tail = w2[pl.ds(edge, w2.shape[0] - edge), :]
        row = lax.broadcasted_iota(jnp.int32, tail.shape, 0)
        w2[pl.ds(edge, w2.shape[0] - edge), :] = jnp.where(row < ffn - edge, tail.astype(f32), 0.0).astype(bf16)

    def gather_wait(b):
        pt_wait(b, 0, 0)
        for k in range(1, far + 1):
            for d in range(2):
                pt_wait(b, d, k)

    def up(b, lo, hi):
        def body(j, carry):
            wj = w1[pl.ds(pl.multiple_of(j * 2 * LANES, 2 * LANES), 2 * LANES), :]
            gu = lax.dot_general(m_all[b], wj, (((1,), (1,)), ((), ())), preferred_element_type=f32)
            gate, upv = gu[:, :LANES], gu[:, LANES:]
            val = gate / (1.0 + jnp.exp(-gate)) * upv
            col = lax.broadcasted_iota(jnp.int32, val.shape, 1) + j * LANES
            act[:, pl.ds(pl.multiple_of(j * LANES, LANES), LANES)] = jnp.where(col < ffn, val, 0.0).astype(bf16)
            return carry
        lax.fori_loop(lo, hi, body, 0)

    def px(b, n):
        cols = pl.ds(n * ncol if isinstance(n, int) else pl.multiple_of(n * ncol, ncol), ncol)
        src = part.at[b, pl.ds(pl.multiple_of(other * chips * rb, chips * rb), chips * rb), cols]
        return rcopy(src, pair_rx.at[b, :, cols], px_send.at[b, n], px_recv.at[b, n], partner)

    def down(b, lo, hi):
        def body(n, carry):
            cols = pl.ds(pl.multiple_of(n * ncol, ncol), ncol)
            part[b, :, cols] = jnp.dot(act[...], w2[:, cols], preferred_element_type=f32).astype(bf16)
            px(b, n).start()
            return carry
        lax.fori_loop(lo, hi, body, 0)

    def pair_sum(b, chip, cols):
        mine = part[b, rows(core, chip), cols].astype(f32)
        return mine + pair_rx[b, pl.ds(pl.multiple_of(chip * rb, rb), rb), cols].astype(f32)

    def rs(b, direction, left_hops, hf):
        cols = pl.ds(hf * half, half)
        return rcopy(rs_tx.at[b, direction, left_hops, :, cols], rs_rx.at[b, direction, left_hops, :, cols],
                     rs_send.at[b, direction, left_hops, hf], rs_recv.at[b, direction, left_hops, hf], nbr[direction])

    def rs_step(b, k):
        for hf in range(2):
            cols = pl.ds(hf * half, half)
            for d in range(2):
                if k == far and hf != d:
                    continue
                val = pair_sum(b, chip_at(1 - d, k), cols)
                if k < far and (k < far - 1 or hf == d):
                    rs(b, d, k, hf).wait_recv()
                    val = val + rs_rx[b, d, k, :, cols].astype(f32)
                rs_tx[b, d, k - 1, :, cols] = val.astype(bf16)
                start(rs(b, d, k - 1, hf))

    def rs_last(b):
        for hf in range(2):
            cols = pl.ds(hf * half, half)
            val = pair_sum(b, z, cols)
            for d in range(2):
                rs(b, d, 0, hf).wait_recv()
                val = val + rs_rx[b, d, 0, :, cols].astype(f32)
            o_ref[pl.ds(b * rb, rb), cols] = (h_ref[pl.ds(b * rb, rb), cols] + val).astype(bf16)

    nblk = width // ncol

    def pair_wait(b):
        for n in range(nblk):
            px(b, n).wait()

    gather_wait(0)
    up(0, 0, fblocks)
    down(0, 0, nblk)
    gather_wait(1)
    pair_wait(0)
    rs_step(0, far)
    cuts = [i * fblocks // 2 for i in range(3)]
    up(1, cuts[0], cuts[1])
    rs_step(0, 3) if far > 3 else None
    up(1, cuts[1], cuts[2])
    rs_step(0, 2)
    down(1, 0, nblk)
    pair_wait(1)
    rs_step(1, far)
    rs_step(0, 1)
    rs_step(1, 3) if far > 3 else None
    rs_last(0)
    rs_step(1, 2)
    rs_step(1, 1)
    rs_last(1)
    for copy in started:
        copy.wait_send()


def mlp_layer(mesh, hidden, mlp_in, w_in, w_out):
    rows, width = mlp_in.shape
    group = mesh.shape['grp']
    chips = group // 2
    far = chips // 2
    rb = rows // 2
    ffn = w_out.shape[0]
    fpad = -(-ffn // LANES) * LANES
    bf16 = jnp.bfloat16
    vmem = pl.BlockSpec(memory_space=pltpu.VMEM)
    hbm = pl.BlockSpec(memory_space=pl.ANY)
    dma = pltpu.SemaphoreType.DMA
    return pl.pallas_call(
        functools.partial(mlp_kernel, chips),
        name='mlp_ring',
        out_shape=jax.ShapeDtypeStruct((rows, width), bf16),
        in_specs=[vmem, vmem, hbm, hbm],
        out_specs=vmem,
        scratch_shapes=[
            pltpu.VMEM((2, group * rb, width), bf16),
            pltpu.VMEM((2 * fpad, width), bf16),
            pltpu.VMEM((fpad, width), bf16),
            pltpu.VMEM((group * rb, fpad), bf16),
            pltpu.VMEM((2, group * rb, width), bf16),
            pltpu.VMEM((2, chips * rb, width), bf16),
            pltpu.VMEM((2, 2, far, rb, width), bf16),
            pltpu.VMEM((2, 2, far, rb, width), bf16),
            dma((2 * fpad // LANES,)), dma,
            dma((2, 2, far)), dma((2, 2, far)),
            dma((2, 2 * far + 1)), dma((2, 2 * far + 1)),
            dma((2, width // 512)), dma((2, width // 512)),
            dma((2, 2, far, 2)), dma((2, 2, far, 2)),
        ],
        compiler_params=pltpu.CompilerParams(collective_id=0, has_side_effects=True, vmem_limit_bytes=60 * 1024 * 1024),
    )(mlp_in, hidden, w_in, w_out)


def solution(mesh):
    row_spec = P(('rep', 'grp'))
    repl_spec = P()

    def local_layer(x_in, seq_len, k_cache, v_cache, gamma_attn, w_qkv, b_qkv, w_proj, gamma_mlp, w_in, w_out):
        hidden, k_out, v_out = attention_block(x_in, seq_len, k_cache, v_cache, gamma_attn, w_qkv, b_qkv, w_proj)
        mlp_in = rms_norm(hidden, gamma_mlp)
        layer_out = mlp_layer(mesh, hidden, mlp_in, w_in, w_out)
        return layer_out, k_out, v_out

    return jax.shard_map(local_layer, mesh=mesh,
                         in_specs=(row_spec, row_spec, row_spec, row_spec, repl_spec, repl_spec, repl_spec,
                                   repl_spec, repl_spec, P(None, 'grp', None), P('grp', None)),
                         out_specs=(row_spec, row_spec, row_spec), check_vma=False)
```

```python
import functools
import math

import jax
import jax.numpy as jnp
from jax import lax
from jax.experimental import pallas as pl
from jax.experimental.pallas import tpu as pltpu
from jax.sharding import PartitionSpec as P

HEAD_DIM = 128
ROPE_BASE = 10000.0
EPS = 1e-5
MESH = pl.DeviceIdType.MESH
LANES = 128


def attn_kernel(len_ref, x_ref, ga_ref, b_ref, gm_ref, w_qkv, w_proj, k_in, v_in, h_out, m_out, k_out, v_out,
                wbuf, kbuf, vbuf, normed, qs, cs, ctx, new, wsem, kv_sem, out_sem):
    f32, bf16 = jnp.float32, jnp.bfloat16
    rows, width = x_ref.shape
    cache = kbuf.shape[1]
    slots, _, ncol = wbuf.shape
    heads = qs.shape[0] // rows
    nq = w_qkv.shape[1] // ncol
    nproj = w_proj.shape[1] // ncol
    per = ncol // HEAD_DIM
    nseq = 4

    def weight(i, slot):
        src = w_qkv.at[:, pl.ds(i * ncol, ncol)] if i < nq else w_proj.at[:, pl.ds((i - nq) * ncol, ncol)]
        return pltpu.make_async_copy(src, wbuf.at[slot], wsem.at[slot])

    def weight_dyn(src, i, slot):
        return pltpu.make_async_copy(src.at[:, pl.ds(pl.multiple_of(i * ncol, ncol), ncol)], wbuf.at[slot], wsem.at[slot])

    def kv(src, dst, i):
        return pltpu.make_async_copy(src.at[pl.ds(i * 8, 8)], dst.at[pl.ds(i * 8, 8)], kv_sem.at[i])

    for i in range(slots):
        weight(i, i).start()

    def normalize(vals, gain):
        mean_sq = jnp.mean(vals * vals, axis=-1, keepdims=True)
        return (vals * lax.rsqrt(mean_sq + EPS) * gain).astype(bf16)

    normed[...] = normalize(x_ref[...].astype(f32), ga_ref[...].astype(f32))

    row = lax.broadcasted_iota(jnp.int32, (rows, HEAD_DIM), 0)
    lane = lax.broadcasted_iota(jnp.int32, (rows, HEAD_DIM), 1)
    rot_dim = HEAD_DIM // 2
    pos = jnp.zeros((rows, HEAD_DIM), jnp.int32)
    for i in range(rows):
        pos = jnp.where(row == i, len_ref[i], pos)
    even = lane % 2 == 0
    freq = jnp.exp((lane // 2 * 2).astype(f32) * (-math.log(ROPE_BASE) / rot_dim))
    angle = pos.astype(f32) * freq
    turned = lane < rot_dim
    cosine = jnp.where(turned, jnp.cos(angle), 1.0)
    sine = jnp.where(turned, jnp.sin(angle), 0.0)
    sine = jnp.where(even, -sine, sine)

    def rotate(vals):
        swapped = jnp.where(even, pltpu.roll(vals, HEAD_DIM - 1, 1), pltpu.roll(vals, 1, 1))
        return vals * cosine + swapped * sine

    def project(lhs, slot):
        return jnp.dot(lhs[...], wbuf[slot], preferred_element_type=f32)

    def refill(i, slot):
        nxt = i + slots
        @pl.when(nxt < nq)
        def _():
            weight_dyn(w_qkv, nxt, slot).start()
        @pl.when(nxt == nq)
        def _():
            for j in range(rows // 8):
                kv(k_in, kbuf, j).start()
                kv(v_in, vbuf, j).start()
        @pl.when(jnp.logical_and(nxt >= nq, nxt < nq + nproj))
        def _():
            weight_dyn(w_proj, nxt - nq, slot).start()

    def query_block(j, carry):
        slot = lax.rem(j, slots)
        weight_dyn(w_qkv, j, slot).wait()
        acc = project(normed, slot) + b_ref[:, pl.ds(pl.multiple_of(j * ncol, ncol), ncol)].astype(f32)
        for i in range(per):
            qs[pl.ds(j * per + i, rows, stride=heads), :] = rotate(acc[:, i * HEAD_DIM:(i + 1) * HEAD_DIM])
        refill(j, slot)
        return carry

    lax.fori_loop(0, nq - 1, query_block, 0)

    last = nq - 1
    weight(last, last % slots).wait()
    acc = project(normed, last % slots) + b_ref[:, pl.ds(last * ncol, ncol)].astype(f32)
    refill(last, last % slots)
    for i in range(4):
        vals = acc[:, i * HEAD_DIM:(i + 1) * HEAD_DIM]
        new[i] = rotate(vals) if i < 2 else vals

    for j in range(rows // 8):
        kv(k_in, kbuf, j).wait()
        kv(v_in, vbuf, j).wait()

    def insert(b, carry):
        length = len_ref[b]
        base = pl.multiple_of(length // 8 * 16, 16)
        at = 2 * length - base
        r16 = lax.broadcasted_iota(jnp.int32, (16, HEAD_DIM), 0)
        for i, buf in ((0, kbuf), (2, vbuf)):
            tile = buf[b, pl.ds(base, 16), :].astype(f32)
            tile = jnp.where(r16 == at, new[i, pl.ds(b, 1), :], tile)
            tile = jnp.where(r16 == at + 1, new[i + 1, pl.ds(b, 1), :], tile)
            buf[b, pl.ds(base, 16), :] = tile.astype(bf16)
        return carry

    lax.fori_loop(0, rows, insert, 0)

    def out_copy(b, i):
        src, dst = ((kbuf, k_out), (vbuf, v_out))[i]
        return pltpu.make_async_copy(src.at[pl.ds(b * nseq, nseq)], dst.at[pl.ds(b * nseq, nseq)], out_sem.at[i])

    srow = lax.broadcasted_iota(jnp.int32, (heads, cache), 0)
    scol = lax.broadcasted_iota(jnp.int32, (heads, cache), 1)
    same_group = (srow // (heads // 2)) == (scol % 2)
    spos = jnp.where(same_group, scol // 2, cache)

    def attend(step, carry):
        for i in range(nseq):
            b = step * nseq + i
            q = qs[pl.ds(pl.multiple_of(b * heads, heads), heads), :].astype(bf16)
            s = lax.dot_general(q, kbuf[b], (((1,), (1,)), ((), ())), preferred_element_type=f32) * HEAD_DIM ** -0.5
            s = jnp.where(spos <= len_ref[b], s, -jnp.inf)
            e = jnp.exp(s - jnp.max(s, axis=-1, keepdims=True))
            p = (e * (1.0 / jnp.sum(e, axis=-1, keepdims=True))).astype(bf16)
            cs[pl.ds(pl.multiple_of(b * heads, heads), heads), :] = jnp.dot(p, vbuf[b], preferred_element_type=f32)
        for i in range(2):
            out_copy(step, i).start()
        return carry

    lax.fori_loop(0, rows // nseq, attend, 0)

    for i in range(heads):
        ctx[:, i * HEAD_DIM:(i + 1) * HEAD_DIM] = cs[pl.ds(i, rows, stride=heads), :].astype(bf16)

    def proj_block(j, carry):
        slot = lax.rem(j + nq, slots)
        cols = pl.ds(pl.multiple_of(j * ncol, ncol), ncol)
        weight_dyn(w_proj, j, slot).wait()
        h_out[:, cols] = x_ref[:, cols].astype(f32) + project(ctx, slot)
        refill(j + nq, slot)
        return carry

    lax.fori_loop(0, nproj, proj_block, 0)
    m_out[...] = normalize(h_out[...], gm_ref[...].astype(f32))

    def drain(step, carry):
        for i in range(2):
            out_copy(step, i).wait()
        return carry

    lax.fori_loop(0, rows // nseq, drain, 0)


def attention_layer(x_in, seq_len, k_cache, v_cache, gamma_attn, w_qkv, b_qkv, w_proj, gamma_mlp):
    rows, width = x_in.shape
    cache_len, kv_heads = k_cache.shape[1], k_cache.shape[2]
    heads = w_proj.shape[0] // HEAD_DIM
    ncol, slots = 512, 6
    f32, bf16 = jnp.float32, jnp.bfloat16
    flat = (rows, cache_len * kv_heads, HEAD_DIM)
    vmem = pl.BlockSpec(memory_space=pltpu.VMEM)
    smem = pl.BlockSpec(memory_space=pltpu.SMEM)
    hbm = pl.BlockSpec(memory_space=pl.ANY)
    dma = pltpu.SemaphoreType.DMA
    hidden, mlp_in, k_out, v_out = pl.pallas_call(
        attn_kernel,
        name='attention',
        out_shape=(jax.ShapeDtypeStruct((rows, width), f32), jax.ShapeDtypeStruct((rows, width), bf16),
                   jax.ShapeDtypeStruct(flat, bf16), jax.ShapeDtypeStruct(flat, bf16)),
        in_specs=[smem, vmem, vmem, vmem, vmem, hbm, hbm, hbm, hbm],
        out_specs=(vmem, vmem, hbm, hbm),
        scratch_shapes=[
            pltpu.VMEM((slots, width, ncol), bf16),
            pltpu.VMEM(flat, bf16), pltpu.VMEM(flat, bf16),
            pltpu.VMEM((rows, width), bf16),
            pltpu.VMEM((rows * heads, HEAD_DIM), f32), pltpu.VMEM((rows * heads, HEAD_DIM), f32),
            pltpu.VMEM((rows, heads * HEAD_DIM), bf16),
            pltpu.VMEM((2 * kv_heads, rows, HEAD_DIM), f32),
            dma((slots,)), dma((rows // 8,)), dma((2,)),
        ],
        compiler_params=pltpu.CompilerParams(vmem_limit_bytes=56 * 1024 * 1024),
    )(seq_len, x_in, gamma_attn.reshape(1, -1), b_qkv.reshape(1, -1), gamma_mlp.reshape(1, -1), w_qkv, w_proj,
      k_cache.reshape(flat), v_cache.reshape(flat))
    return hidden, mlp_in, k_out.reshape(k_cache.shape), v_out.reshape(v_cache.shape)


def mlp_kernel(chips, m_ref, h_ref, w_in_ref, w_out_ref, o_ref, m_all, w1, w2, act, part, pair_rx, rs_rx, rs_tx,
               w1_sem, w2_sem, ag_send, ag_recv, pt_send, pt_recv, px_send, px_recv, rs_send, rs_recv):
    f32, bf16 = jnp.float32, jnp.bfloat16
    width = m_ref.shape[1]
    half = width // 2
    rb = m_ref.shape[0] // 2
    ffn = w_out_ref.shape[0]
    fblocks = w2.shape[0] // LANES
    far = chips // 2
    ncol = 512

    me = lax.axis_index('grp')
    z, core = me // 2, me % 2
    other = 1 - core
    right = lax.rem(z + 1, chips) * 2 + core
    left = lax.rem(z + chips - 1, chips) * 2 + core
    partner = z * 2 + other
    nbr = (right, left)

    def chip_at(direction, k):
        return lax.rem(z + (chips - k if direction == 0 else k), chips)

    def rows(c, chip):
        return pl.ds(pl.multiple_of((c * chips + chip) * rb, rb), rb)

    def rcopy(src, dst, ssem, rsem, dev):
        return pltpu.make_async_remote_copy(src_ref=src, dst_ref=dst, send_sem=ssem, recv_sem=rsem,
                                            device_id={'grp': dev}, device_id_type=MESH)

    w_copies = []
    for j in range(fblocks):
        n = min(LANES, ffn - j * LANES)
        for c in range(2):
            w_copies.append(pltpu.make_async_copy(w_in_ref.at[c, pl.ds(j * LANES, n), :],
                                                  w1.at[pl.ds((2 * j + c) * LANES, n), :], w1_sem.at[2 * j + c]))
    w_copies.append(pltpu.make_async_copy(w_out_ref, w2.at[pl.ds(0, ffn), :], w2_sem))

    barrier = pltpu.get_barrier_semaphore()
    for dev in (right, left, partner):
        pl.semaphore_signal(barrier, inc=1, device_id={'grp': dev}, device_id_type=MESH)
    pl.semaphore_wait(barrier, 3)

    def ag_cols(direction, k):
        return pl.ds(direction * half, half) if k == far else pl.ds(0, width)

    def ag(b, direction, k):
        cols = ag_cols(direction, k)
        if k == 1:
            src = m_ref.at[pl.ds(b * rb, rb), :]
            sent = z
        else:
            sent = chip_at(direction, k - 1)
            src = m_all.at[b, rows(core, sent), cols]
        return rcopy(src, m_all.at[b, rows(core, sent), cols], ag_send.at[b, direction, k - 1],
                     ag_recv.at[b, direction, k - 1], nbr[direction])

    def ag_wait(b, direction, k):
        got = m_all.at[b, rows(core, chip_at(direction, k)), ag_cols(direction, k)]
        rcopy(got, got, ag_send.at[b, direction, k - 1], ag_recv.at[b, direction, k - 1], nbr[direction]).wait_recv()

    def pt(b, direction, k):
        if k == 0:
            blk = m_all.at[b, rows(core, z), :]
            return rcopy(m_ref.at[pl.ds(b * rb, rb), :], blk, pt_send.at[b, 0], pt_recv.at[b, 0], partner)
        slot = 1 + direction * far + k - 1
        blk = m_all.at[b, rows(core, chip_at(direction, k)), ag_cols(direction, k)]
        return rcopy(blk, blk, pt_send.at[b, slot], pt_recv.at[b, slot], partner)

    def pt_wait(b, direction, k):
        if k == 0:
            blk = m_all.at[b, rows(other, z), :]
            return rcopy(blk, blk, pt_send.at[b, 0], pt_recv.at[b, 0], partner).wait_recv()
        slot = 1 + direction * far + k - 1
        blk = m_all.at[b, rows(other, chip_at(direction, k)), ag_cols(direction, k)]
        return rcopy(blk, blk, pt_send.at[b, slot], pt_recv.at[b, slot], partner).wait_recv()

    started = []

    def start(copy):
        copy.start()
        started.append(copy)

    for b in range(2):
        for d in range(2):
            start(ag(b, d, 1))
    for b in range(2):
        start(pt(b, 0, 0))
    for copy in w_copies:
        copy.start()
    for b in range(2):
        m_all[b, rows(core, z), :] = m_ref[pl.ds(b * rb, rb), :]
    for k in range(1, far + 1):
        for b in range(2):
            for d in range(2):
                ag_wait(b, d, k)
                if k < far:
                    start(ag(b, d, k + 1))
                start(pt(b, d, k))
    for copy in w_copies:
        copy.wait()
    edge = ffn // 16 * 16
    if edge < w2.shape[0]:
        tail = w2[pl.ds(edge, w2.shape[0] - edge), :]
        row = lax.broadcasted_iota(jnp.int32, tail.shape, 0)
        w2[pl.ds(edge, w2.shape[0] - edge), :] = jnp.where(row < ffn - edge, tail.astype(f32), 0.0).astype(bf16)

    def gather_wait(b):
        pt_wait(b, 0, 0)
        for k in range(1, far + 1):
            for d in range(2):
                pt_wait(b, d, k)

    def up(b, lo, hi):
        def body(j, carry):
            wj = w1[pl.ds(pl.multiple_of(j * 2 * LANES, 2 * LANES), 2 * LANES), :]
            gu = lax.dot_general(m_all[b], wj, (((1,), (1,)), ((), ())), preferred_element_type=f32)
            gate, upv = gu[:, :LANES], gu[:, LANES:]
            val = gate / (1.0 + jnp.exp(-gate)) * upv
            col = lax.broadcasted_iota(jnp.int32, val.shape, 1) + j * LANES
            act[:, pl.ds(pl.multiple_of(j * LANES, LANES), LANES)] = jnp.where(col < ffn, val, 0.0).astype(bf16)
            return carry
        lax.fori_loop(lo, hi, body, 0)

    def px(b, n):
        cols = pl.ds(n * ncol if isinstance(n, int) else pl.multiple_of(n * ncol, ncol), ncol)
        src = part.at[b, pl.ds(pl.multiple_of(other * chips * rb, chips * rb), chips * rb), cols]
        return rcopy(src, pair_rx.at[b, :, cols], px_send.at[b, n], px_recv.at[b, n], partner)

    def down(b, lo, hi):
        def body(n, carry):
            cols = pl.ds(pl.multiple_of(n * ncol, ncol), ncol)
            part[b, :, cols] = jnp.dot(act[...], w2[:, cols], preferred_element_type=f32).astype(bf16)
            px(b, n).start()
            return carry
        lax.fori_loop(lo, hi, body, 0)

    def pair_sum(b, chip, cols):
        mine = part[b, rows(core, chip), cols].astype(f32)
        return mine + pair_rx[b, pl.ds(pl.multiple_of(chip * rb, rb), rb), cols].astype(f32)

    def rs(b, direction, left_hops, hf):
        cols = pl.ds(hf * half, half)
        return rcopy(rs_tx.at[b, direction, left_hops, :, cols], rs_rx.at[b, direction, left_hops, :, cols],
                     rs_send.at[b, direction, left_hops, hf], rs_recv.at[b, direction, left_hops, hf], nbr[direction])

    def rs_step(b, k):
        for hf in range(2):
            cols = pl.ds(hf * half, half)
            for d in range(2):
                if k == far and hf != d:
                    continue
                val = pair_sum(b, chip_at(1 - d, k), cols)
                if k < far and (k < far - 1 or hf == d):
                    rs(b, d, k, hf).wait_recv()
                    val = val + rs_rx[b, d, k, :, cols].astype(f32)
                rs_tx[b, d, k - 1, :, cols] = val.astype(bf16)
                start(rs(b, d, k - 1, hf))

    def rs_last(b):
        for hf in range(2):
            cols = pl.ds(hf * half, half)
            val = pair_sum(b, z, cols)
            for d in range(2):
                rs(b, d, 0, hf).wait_recv()
                val = val + rs_rx[b, d, 0, :, cols].astype(f32)
            o_ref[pl.ds(b * rb, rb), cols] = (h_ref[pl.ds(b * rb, rb), cols] + val).astype(bf16)

    nblk = width // ncol

    def pair_wait(b):
        for n in range(nblk):
            px(b, n).wait()

    gather_wait(0)
    up(0, 0, fblocks)
    down(0, 0, nblk)
    gather_wait(1)
    pair_wait(0)
    rs_step(0, far)
    cuts = [i * fblocks // 2 for i in range(3)]
    up(1, cuts[0], cuts[1])
    rs_step(0, 3) if far > 3 else None
    up(1, cuts[1], cuts[2])
    rs_step(0, 2)
    down(1, 0, nblk)
    pair_wait(1)
    rs_step(1, far)
    rs_step(0, 1)
    rs_step(1, 3) if far > 3 else None
    rs_last(0)
    rs_step(1, 2)
    rs_step(1, 1)
    rs_last(1)
    for copy in started:
        copy.wait_send()


def mlp_layer(mesh, hidden, mlp_in, w_in, w_out):
    rows, width = mlp_in.shape
    group = mesh.shape['grp']
    chips = group // 2
    far = chips // 2
    rb = rows // 2
    ffn = w_out.shape[0]
    fpad = -(-ffn // LANES) * LANES
    bf16 = jnp.bfloat16
    vmem = pl.BlockSpec(memory_space=pltpu.VMEM)
    hbm = pl.BlockSpec(memory_space=pl.ANY)
    dma = pltpu.SemaphoreType.DMA
    return pl.pallas_call(
        functools.partial(mlp_kernel, chips),
        name='mlp_ring',
        out_shape=jax.ShapeDtypeStruct((rows, width), bf16),
        in_specs=[vmem, vmem, hbm, hbm],
        out_specs=vmem,
        scratch_shapes=[
            pltpu.VMEM((2, group * rb, width), bf16),
            pltpu.VMEM((2 * fpad, width), bf16),
            pltpu.VMEM((fpad, width), bf16),
            pltpu.VMEM((group * rb, fpad), bf16),
            pltpu.VMEM((2, group * rb, width), bf16),
            pltpu.VMEM((2, chips * rb, width), bf16),
            pltpu.VMEM((2, 2, far, rb, width), bf16),
            pltpu.VMEM((2, 2, far, rb, width), bf16),
            dma((2 * fpad // LANES,)), dma,
            dma((2, 2, far)), dma((2, 2, far)),
            dma((2, 2 * far + 1)), dma((2, 2 * far + 1)),
            dma((2, width // 512)), dma((2, width // 512)),
            dma((2, 2, far, 2)), dma((2, 2, far, 2)),
        ],
        compiler_params=pltpu.CompilerParams(collective_id=0, has_side_effects=True, vmem_limit_bytes=60 * 1024 * 1024),
    )(mlp_in, hidden, w_in, w_out)


def solution(mesh):
    row_spec = P(('rep', 'grp'))
    repl_spec = P()

    def local_layer(x_in, seq_len, k_cache, v_cache, gamma_attn, w_qkv, b_qkv, w_proj, gamma_mlp, w_in, w_out):
        hidden, mlp_in, k_out, v_out = attention_layer(x_in, seq_len, k_cache, v_cache, gamma_attn, w_qkv, b_qkv, w_proj,
                                                       gamma_mlp)
        layer_out = mlp_layer(mesh, hidden, mlp_in, w_in, w_out)
        return layer_out, k_out, v_out

    return jax.shard_map(local_layer, mesh=mesh,
                         in_specs=(row_spec, row_spec, row_spec, row_spec, repl_spec, repl_spec, repl_spec,
                                   repl_spec, repl_spec, P(None, 'grp', None), P('grp', None)),
                         out_specs=(row_spec, row_spec, row_spec), check_vma=False)
```

```python
import functools
import math

import jax
import jax.numpy as jnp
from jax import lax
from jax.experimental import pallas as pl
from jax.experimental.pallas import tpu as pltpu
from jax.sharding import PartitionSpec as P

HEAD_DIM = 128
ROPE_BASE = 10000.0
EPS = 1e-5
MESH = pl.DeviceIdType.MESH
LANES = 128
PIECES = 4


def attn_kernel(len_ref, x_ref, ga_ref, b_ref, gm_ref, w_qkv, w_proj, k_in, v_in, h_out, m_out, k_out, v_out,
                wbuf, kbuf, vbuf, normed, qs, cs, ctx, new, wsem, kv_sem, out_sem):
    f32, bf16 = jnp.float32, jnp.bfloat16
    rows, width = x_ref.shape
    cache = kbuf.shape[1]
    slots, _, ncol = wbuf.shape
    heads = qs.shape[0] // rows
    nq = w_qkv.shape[1] // ncol
    nproj = w_proj.shape[1] // ncol
    per = ncol // HEAD_DIM
    nseq = 8

    def weight(i, slot):
        src = w_qkv.at[:, pl.ds(i * ncol, ncol)] if i < nq else w_proj.at[:, pl.ds((i - nq) * ncol, ncol)]
        return pltpu.make_async_copy(src, wbuf.at[slot], wsem.at[slot])

    def weight_dyn(src, i, slot):
        return pltpu.make_async_copy(src.at[:, pl.ds(pl.multiple_of(i * ncol, ncol), ncol)], wbuf.at[slot], wsem.at[slot])

    def kv(src, dst, i):
        return pltpu.make_async_copy(src.at[pl.ds(i * 8, 8)], dst.at[pl.ds(i * 8, 8)], kv_sem.at[i])

    for i in range(slots):
        weight(i, i).start()

    def normalize(vals, gain):
        mean_sq = jnp.mean(vals * vals, axis=-1, keepdims=True)
        return (vals * lax.rsqrt(mean_sq + EPS) * gain).astype(bf16)

    normed[...] = normalize(x_ref[...].astype(f32), ga_ref[...].astype(f32)[None, :])

    row = lax.broadcasted_iota(jnp.int32, (rows, HEAD_DIM), 0)
    lane = lax.broadcasted_iota(jnp.int32, (rows, HEAD_DIM), 1)
    rot_dim = HEAD_DIM // 2
    pos = jnp.zeros((rows, HEAD_DIM), jnp.int32)
    for i in range(rows):
        pos = jnp.where(row == i, len_ref[i], pos)
    even = lane % 2 == 0
    freq = jnp.exp((lane // 2 * 2).astype(f32) * (-math.log(ROPE_BASE) / rot_dim))
    angle = pos.astype(f32) * freq
    turned = lane < rot_dim
    cosine = jnp.where(turned, jnp.cos(angle), 1.0)
    sine = jnp.where(turned, jnp.sin(angle), 0.0)
    sine = jnp.where(even, -sine, sine)

    def rotate(vals):
        swapped = jnp.where(even, pltpu.roll(vals, HEAD_DIM - 1, 1), pltpu.roll(vals, 1, 1))
        return vals * cosine + swapped * sine

    def project(lhs, slot):
        return jnp.dot(lhs[...], wbuf[slot], preferred_element_type=f32)

    def refill(i, slot):
        nxt = i + slots
        @pl.when(nxt < nq)
        def _():
            weight_dyn(w_qkv, nxt, slot).start()
        @pl.when(nxt == nq)
        def _():
            for j in range(rows // 8):
                kv(k_in, kbuf, j).start()
                kv(v_in, vbuf, j).start()
        @pl.when(jnp.logical_and(nxt >= nq, nxt < nq + nproj))
        def _():
            weight_dyn(w_proj, nxt - nq, slot).start()

    def query_block(j, carry):
        slot = lax.rem(j, slots)
        weight_dyn(w_qkv, j, slot).wait()
        acc = project(normed, slot) + b_ref[pl.ds(pl.multiple_of(j * ncol, ncol), ncol)].astype(f32)[None, :]
        for i in range(per):
            qs[pl.ds(j * per + i, rows, stride=heads), :] = rotate(acc[:, i * HEAD_DIM:(i + 1) * HEAD_DIM])
        refill(j, slot)
        return carry

    with jax.named_scope('qkv'):
        lax.fori_loop(0, nq - 1, query_block, 0)

    last = nq - 1
    weight(last, last % slots).wait()
    acc = project(normed, last % slots) + b_ref[pl.ds(last * ncol, ncol)].astype(f32)[None, :]
    refill(last, last % slots)
    for i in range(4):
        vals = acc[:, i * HEAD_DIM:(i + 1) * HEAD_DIM]
        new[i] = rotate(vals) if i < 2 else vals

    for j in range(rows // 8):
        kv(k_in, kbuf, j).wait()
        kv(v_in, vbuf, j).wait()

    def insert(b, carry):
        length = len_ref[b]
        base = pl.multiple_of(length // 8 * 16, 16)
        at = 2 * length - base
        r16 = lax.broadcasted_iota(jnp.int32, (16, HEAD_DIM), 0)
        for i, buf in ((0, kbuf), (2, vbuf)):
            tile = buf[b, pl.ds(base, 16), :].astype(f32)
            tile = jnp.where(r16 == at, new[i, pl.ds(b, 1), :], tile)
            tile = jnp.where(r16 == at + 1, new[i + 1, pl.ds(b, 1), :], tile)
            buf[b, pl.ds(base, 16), :] = tile.astype(bf16)
        return carry

    with jax.named_scope('insert'):
        lax.fori_loop(0, rows, insert, 0)

    def out_copy(b, i):
        src, dst = ((kbuf, k_out), (vbuf, v_out))[i]
        return pltpu.make_async_copy(src.at[pl.ds(b * nseq, nseq)], dst.at[pl.ds(b * nseq, nseq)], out_sem.at[i])

    srow = lax.broadcasted_iota(jnp.int32, (heads, cache), 0)
    scol = lax.broadcasted_iota(jnp.int32, (heads, cache), 1)
    same_group = (srow // (heads // 2)) == (scol % 2)
    spos = jnp.where(same_group, scol // 2, cache)

    def attend(step, carry):
        seqs = [step * nseq + i for i in range(nseq)]
        scores = []
        for b in seqs:
            q = qs[pl.ds(pl.multiple_of(b * heads, heads), heads), :].astype(bf16)
            scores.append(lax.dot_general(q, kbuf[b], (((1,), (1,)), ((), ())), preferred_element_type=f32))
        probs = []
        for b, s in zip(seqs, scores):
            s = jnp.where(spos <= len_ref[b], s * HEAD_DIM ** -0.5, -jnp.inf)
            e = jnp.exp(s - jnp.max(s, axis=-1, keepdims=True))
            probs.append((e * (1.0 / jnp.sum(e, axis=-1, keepdims=True))).astype(bf16))
        for b, p in zip(seqs, probs):
            cs[pl.ds(pl.multiple_of(b * heads, heads), heads), :] = jnp.dot(p, vbuf[b], preferred_element_type=f32)
        for i in range(2):
            out_copy(step, i).start()
        return carry

    with jax.named_scope('attend'):
        lax.fori_loop(0, rows // nseq, attend, 0)

    for i in range(heads):
        ctx[:, i * HEAD_DIM:(i + 1) * HEAD_DIM] = cs[pl.ds(i, rows, stride=heads), :].astype(bf16)

    def proj_block(j, carry):
        slot = lax.rem(j + nq, slots)
        cols = pl.ds(pl.multiple_of(j * ncol, ncol), ncol)
        weight_dyn(w_proj, j, slot).wait()
        h_out[:, cols] = x_ref[:, cols].astype(f32) + project(ctx, slot)
        refill(j + nq, slot)
        return carry

    with jax.named_scope('proj'):
        lax.fori_loop(0, nproj, proj_block, 0)
    m_out[...] = normalize(h_out[...], gm_ref[...].astype(f32)[None, :])

    def drain(step, carry):
        for i in range(2):
            out_copy(step, i).wait()
        return carry

    with jax.named_scope('drain'):
        lax.fori_loop(0, rows // nseq, drain, 0)


def attention_layer(x_in, seq_len, k_cache, v_cache, gamma_attn, w_qkv, b_qkv, w_proj, gamma_mlp):
    rows, width = x_in.shape
    cache_len, kv_heads = k_cache.shape[1], k_cache.shape[2]
    heads = w_proj.shape[0] // HEAD_DIM
    ncol, slots = 512, 6
    f32, bf16 = jnp.float32, jnp.bfloat16
    flat = (rows, cache_len * kv_heads, HEAD_DIM)
    vmem = pl.BlockSpec(memory_space=pltpu.VMEM)
    smem = pl.BlockSpec(memory_space=pltpu.SMEM)
    hbm = pl.BlockSpec(memory_space=pl.ANY)
    dma = pltpu.SemaphoreType.DMA
    hidden, mlp_in, k_out, v_out = pl.pallas_call(
        attn_kernel,
        name='attention',
        out_shape=(jax.ShapeDtypeStruct((rows, width), f32), jax.ShapeDtypeStruct((rows, width), bf16),
                   jax.ShapeDtypeStruct(flat, bf16), jax.ShapeDtypeStruct(flat, bf16)),
        in_specs=[smem, vmem, vmem, vmem, vmem, hbm, hbm, hbm, hbm],
        out_specs=(vmem, vmem, hbm, hbm),
        scratch_shapes=[
            pltpu.VMEM((slots, width, ncol), bf16),
            pltpu.VMEM(flat, bf16), pltpu.VMEM(flat, bf16),
            pltpu.VMEM((rows, width), bf16),
            pltpu.VMEM((rows * heads, HEAD_DIM), f32), pltpu.VMEM((rows * heads, HEAD_DIM), f32),
            pltpu.VMEM((rows, heads * HEAD_DIM), bf16),
            pltpu.VMEM((2 * kv_heads, rows, HEAD_DIM), f32),
            dma((slots,)), dma((rows // 8,)), dma((2,)),
        ],
        compiler_params=pltpu.CompilerParams(vmem_limit_bytes=56 * 1024 * 1024),
    )(seq_len, x_in, gamma_attn, b_qkv, gamma_mlp, w_qkv, w_proj,
      k_cache.reshape(flat), v_cache.reshape(flat))
    return hidden, mlp_in, k_out.reshape(k_cache.shape), v_out.reshape(v_cache.shape)


def mlp_kernel(chips, m_ref, h_ref, w_in_ref, w_out_ref, o_ref, m_all, w1, w2, act, part, pair_rx, rs_rx, rs_tx,
               w1_sem, w2_sem, send_sem, ag_recv, pt_recv, px_recv, rs_recv):
    f32, bf16 = jnp.float32, jnp.bfloat16
    width = m_ref.shape[1]
    rb = m_ref.shape[0] // 2
    ffn = w_out_ref.shape[0]
    fblocks = w2.shape[0] // LANES
    far = chips // 2
    pw = width // PIECES

    me = lax.axis_index('grp')
    z, core = me // 2, me % 2
    other = 1 - core
    right = lax.rem(z + 1, chips) * 2 + core
    left = lax.rem(z + chips - 1, chips) * 2 + core
    partner = z * 2 + other
    nbr = (right, left)

    def chip_at(direction, k):
        return lax.rem(z + (chips - k if direction == 0 else k), chips)

    def rows(c, chip):
        return pl.ds(pl.multiple_of((c * chips + chip) * rb, rb), rb)

    def core_rows(c):
        return pl.ds(pl.multiple_of(c * chips * rb, chips * rb), chips * rb)

    def cols(q):
        return pl.ds(q * pw, pw)

    def rcopy(src, dst, ssem, rsem, dev):
        return pltpu.make_async_remote_copy(src_ref=src, dst_ref=dst, send_sem=ssem, recv_sem=rsem,
                                            device_id={'grp': dev}, device_id_type=MESH)

    w_copies = []
    for j in range(fblocks):
        n = min(LANES, ffn - j * LANES)
        for c in range(2):
            w_copies.append(pltpu.make_async_copy(w_in_ref.at[c, pl.ds(j * LANES, n), :],
                                                  w1.at[pl.ds((2 * j + c) * LANES, n), :], w1_sem.at[2 * j + c]))
    w_copies.append(pltpu.make_async_copy(w_out_ref, w2.at[pl.ds(0, ffn), :], w2_sem))

    barrier = pltpu.get_barrier_semaphore()
    with jax.named_scope('mbar'):
        for dev in (right, left, partner):
            pl.semaphore_signal(barrier, inc=1, device_id={'grp': dev}, device_id_type=MESH)
        pl.semaphore_wait(barrier, 3)

    def on_path(d, k, q):
        return k < far or (k == far and q % 2 == d)

    def ag_send(b, d, k, q):
        if k == 1:
            src = m_ref.at[pl.ds(b * rb, rb), cols(q)]
            sent = z
        else:
            sent = chip_at(d, k - 1)
            src = m_all.at[b, rows(core, sent), cols(q)]
        rcopy(src, m_all.at[b, rows(core, sent), cols(q)], send_sem.at[0], ag_recv.at[b, d, k - 1, q], nbr[d]).start()

    def ag_step(b, k, q):
        for d in range(2):
            if not on_path(d, k, q):
                continue
            got = m_all.at[b, rows(core, chip_at(d, k)), cols(q)]
            rcopy(got, got, send_sem.at[0], ag_recv.at[b, d, k - 1, q], nbr[d]).wait_recv()
            if on_path(d, k + 1, q):
                ag_send(b, d, k + 1, q)
            rcopy(got, got, send_sem.at[1], pt_recv.at[b], partner).start()

    def ag_begin(b):
        for q in range(PIECES):
            for d in range(2):
                ag_send(b, d, 1, q)
        own = m_ref.at[pl.ds(b * rb, rb), :]
        rcopy(own, m_all.at[b, rows(core, z), :], send_sem.at[1], pt_recv.at[b], partner).start()

    def gather_wait(b):
        got = m_all.at[b, core_rows(other), :]
        rcopy(got, got, send_sem.at[1], pt_recv.at[b], partner).wait_recv()

    def up(b, lo, hi):
        gu = lax.dot_general(m_all[b], w1[2 * lo * LANES:2 * hi * LANES, :], (((1,), (1,)), ((), ())),
                             preferred_element_type=f32)
        for j in range(lo, hi):
            at = 2 * (j - lo) * LANES
            gate, upv = gu[:, at:at + LANES], gu[:, at + LANES:at + 2 * LANES]
            val = gate / (1.0 + jnp.exp(-gate)) * upv
            if (j + 1) * LANES > ffn:
                col = lax.broadcasted_iota(jnp.int32, val.shape, 1) + j * LANES
                val = jnp.where(col < ffn, val, 0.0)
            act[:, j * LANES:(j + 1) * LANES] = val.astype(bf16)

    def px(b, q):
        return rcopy(part.at[b, core_rows(other), cols(q)], pair_rx.at[b, :, cols(q)], send_sem.at[2],
                     px_recv.at[b, q], partner)

    def down(b, q):
        part[b, :, q * pw:(q + 1) * pw] = jnp.dot(act[...], w2[:, q * pw:(q + 1) * pw],
                                                  preferred_element_type=f32).astype(bf16)
        px(b, q).start()

    def pair_sum(b, chip, q):
        mine = part[b, rows(core, chip), cols(q)].astype(f32)
        return mine + pair_rx[b, pl.ds(pl.multiple_of(chip * rb, rb), rb), cols(q)].astype(f32)

    def rs(b, d, k, q):
        return rcopy(rs_tx.at[b, d, k, :, cols(q)], rs_rx.at[b, d, k, :, cols(q)], send_sem.at[3],
                     rs_recv.at[b, d, k, q], nbr[d])

    def rs_send(b, d, k, q):
        val = pair_sum(b, chip_at(1 - d, k), q)
        if on_path(d, k + 1, q):
            rs(b, d, k, q).wait_recv()
            val = val + rs_rx[b, d, k, :, cols(q)].astype(f32)
        rs_tx[b, d, k - 1, :, cols(q)] = val.astype(bf16)
        rs(b, d, k - 1, q).start()

    def rs_first(b, q):
        px(b, q).wait_recv()
        rs_send(b, q % 2, far, q)
        rs_send(b, 1 - q % 2, far - 1, q)

    def rs_later(b):
        yield [(q % 2, far - 1, q) for q in range(PIECES)]
        for k in range(far - 2, 0, -1):
            yield [(1 - q % 2, k, q) for q in range(PIECES)]
            yield [(q % 2, k, q) for q in range(PIECES)]

    def rs_last(b):
        for q in range(PIECES):
            val = pair_sum(b, z, q)
            for d in range(2):
                rs(b, d, 0, q).wait_recv()
                val = val + rs_rx[b, d, 0, :, cols(q)].astype(f32)
            o_ref[pl.ds(b * rb, rb), cols(q)] = (h_ref[pl.ds(b * rb, rb), cols(q)] + val).astype(bf16)

    ag_begin(0)
    for copy in w_copies:
        copy.start()
    for b in range(2):
        m_all[b, rows(core, z), :] = m_ref[pl.ds(b * rb, rb), :]
    with jax.named_scope('ag0'):
        for k in range(1, far):
            for q in range(PIECES):
                ag_step(0, k, q)
    with jax.named_scope('ag0_far'):
        ag_begin(1)
        for q in range(PIECES):
            ag_step(0, far, q)
    with jax.named_scope('gwait0'):
        for copy in w_copies:
            copy.wait()
        gather_wait(0)
    edge = ffn // 16 * 16
    if edge < w2.shape[0]:
        tail = w2[edge:, :]
        row = lax.broadcasted_iota(jnp.int32, tail.shape, 0)
        w2[edge:, :] = jnp.where(row < ffn - edge, tail.astype(f32), 0.0).astype(bf16)

    parts = [(lo, min(lo + 2, fblocks)) for lo in range(0, fblocks, 2)]
    nseg = len(parts) + PIECES

    def mlp(b, between):
        for i in range(nseg):
            with jax.named_scope(f'b{b}_{i}'):
                for fn in between[i]:
                    fn()
            with jax.named_scope(f's{b}_{i}'):
                if i < len(parts):
                    up(b, *parts[i])
                else:
                    down(b, i - len(parts))
        with jax.named_scope(f'b{b}_{nseg}'):
            for fn in between[nseg]:
                fn()

    def spread(items, lo, hi):
        slots = [[] for _ in range(nseg + 1)]
        n = hi - lo + 1
        for i, item in enumerate(items):
            slots[lo + i * n // len(items)].append(item)
        return slots

    ag_items = [functools.partial(ag_step, 1, k, q) for k in range(1, far + 1) for q in range(PIECES)]
    slots0 = spread(ag_items, 0, nseg - 1)
    for q in range(PIECES):
        slots0[min(len(parts) + q + 2, nseg)].append(functools.partial(rs_first, 0, q))
    mlp(0, slots0)
    with jax.named_scope('gwait1'):
        gather_wait(1)

    def group(b, items):
        def run():
            for d, k, q in items:
                rs_send(b, d, k, q)
        return run

    slots1 = spread([group(0, g) for g in rs_later(0)], 1, nseg - 2)
    slots1[nseg].append(functools.partial(rs_last, 0))
    for q in range(PIECES):
        slots1[min(len(parts) + q + 2, nseg)].append(functools.partial(rs_first, 1, q))
    mlp(1, slots1)
    for i, g in enumerate(rs_later(1)):
        with jax.named_scope(f'rs1_{i}'):
            group(1, g)()
    with jax.named_scope('last1'):
        rs_last(1)

    with jax.named_scope('sends'):
        ring_rows = 2 * (2 * far - 1) * rb
        for i, ref in ((0, part.at[0, pl.ds(0, ring_rows), :]), (1, part.at[0]), (2, part.at[0]),
                       (3, part.at[0, pl.ds(0, ring_rows), :])):
            pltpu.make_async_copy(ref, ref, send_sem.at[i]).wait()


def mlp_layer(mesh, hidden, mlp_in, w_in, w_out):
    rows, width = mlp_in.shape
    group = mesh.shape['grp']
    chips = group // 2
    far = chips // 2
    rb = rows // 2
    ffn = w_out.shape[0]
    fpad = -(-ffn // LANES) * LANES
    bf16 = jnp.bfloat16
    vmem = pl.BlockSpec(memory_space=pltpu.VMEM)
    hbm = pl.BlockSpec(memory_space=pl.ANY)
    dma = pltpu.SemaphoreType.DMA
    return pl.pallas_call(
        functools.partial(mlp_kernel, chips),
        name='mlp_ring',
        out_shape=jax.ShapeDtypeStruct((rows, width), bf16),
        in_specs=[vmem, vmem, hbm, hbm],
        out_specs=vmem,
        scratch_shapes=[
            pltpu.VMEM((2, group * rb, width), bf16),
            pltpu.VMEM((2 * fpad, width), bf16),
            pltpu.VMEM((fpad, width), bf16),
            pltpu.VMEM((group * rb, fpad), bf16),
            pltpu.VMEM((2, group * rb, width), bf16),
            pltpu.VMEM((2, chips * rb, width), bf16),
            pltpu.VMEM((2, 2, far, rb, width), bf16),
            pltpu.VMEM((2, 2, far, rb, width), bf16),
            dma((2 * fpad // LANES,)), dma, dma((4,)),
            dma((2, 2, far, PIECES)), dma((2,)), dma((2, PIECES)), dma((2, 2, far, PIECES)),
        ],
        compiler_params=pltpu.CompilerParams(collective_id=0, has_side_effects=True, vmem_limit_bytes=60 * 1024 * 1024),
    )(mlp_in, hidden, w_in, w_out)


def solution(mesh):
    row_spec = P(('rep', 'grp'))
    repl_spec = P()

    def local_layer(x_in, seq_len, k_cache, v_cache, gamma_attn, w_qkv, b_qkv, w_proj, gamma_mlp, w_in, w_out):
        hidden, mlp_in, k_out, v_out = attention_layer(x_in, seq_len, k_cache, v_cache, gamma_attn, w_qkv, b_qkv, w_proj,
                                                       gamma_mlp)
        layer_out = mlp_layer(mesh, hidden, mlp_in, w_in, w_out)
        return layer_out, k_out, v_out

    return jax.shard_map(local_layer, mesh=mesh,
                         in_specs=(row_spec, row_spec, row_spec, row_spec, repl_spec, repl_spec, repl_spec,
                                   repl_spec, repl_spec, P(None, 'grp', None), P('grp', None)),
                         out_specs=(row_spec, row_spec, row_spec), check_vma=False)
```
